32 devices in a mesh: grp: 2 (over x), tm: 16 (over z, y, core).
Axes of the slice: x: 2, y: 2, z: 4, core: 2. Of those that a mesh axis runs over, the one named last changes fastest.
Arguments:
- video_features: bfloat16 [32, 24, 8, 256], P('tm', 'grp'), parts along dimension 1, may hold values from -6 to 6
- cotangent: bfloat16 [32, 24, 8, 256], P('tm', 'grp'), parts along dimension 1, may hold values from -6 to 6
- encoder_weight: bfloat16 [6912, 256], replicated, may hold values from -0.078125 to 0.078125
- down_weight: bfloat16 [2048, 256], replicated, may hold values from -0.125 to 0.125
- coarse_weight: bfloat16 [768, 256], replicated, may hold values from -0.21875 to 0.21875
- up_weight: bfloat16 [256, 2048], replicated, may hold values from -0.375 to 0.375
- decoder_weight: bfloat16 [6912, 256], replicated, may hold values from -0.078125 to 0.078125
- levels: int32 [256], replicated, may hold values from 3 to 8
Outputs:
- video_grad: bfloat16 [32, 24, 8, 256], P('tm', 'grp'), parts along dimension 1
- latent_codes: bfloat16 [16, 12, 4, 256], P('tm', 'grp'), parts along dimension 1
- down_grad: float32 [4096, 256], P(('grp', 'tm')), parts along dimension 0
- coarse_grad: float32 [1536, 256], P(('grp', 'tm')), parts along dimension 0
- up_grad: float32 [512, 2048], P(('grp', 'tm')), parts along dimension 0
The draws below stay inside these ranges and needn't reach their ends.
There are 2 independent parts, one for each index of `grp`. The reference program is written for one: setup_inputs(seed, part) draws one part's arguments, and reference() takes and returns one part's arrays. A program takes and returns all parts, laid end to end along the dimension named above; an argument that names none is the same for every part. Nothing has to cross between parts.
All inputs are finite; a program needn't handle non-finite values.
Results may differ from the reference program's by a relative error of at most 0.018.
The reference program's roundings to bfloat16 on the way count: a program that leaves them out, or rounds other values in their place, can miss the bound.
Values may be sent and summed in bfloat16 or wider, within the bound.
A program may use at most 64 MiB of HBM per device.

```python
import math
import jax
import jax.numpy as jnp
from jax import lax

C = 256
H = 12
W = 8
T_SIZE = 32


def place_ends(drawn, key, least, largest):
    extent = drawn.shape
    spot = [jax.random.randint(jax.random.fold_in(key, axis), (), 0, extent[axis]) for axis in range(len(extent))]
    drawn = drawn.at[tuple(spot)].set(least)
    longest = extent.index(max(extent))
    spot[longest] = (spot[longest] + 1) % extent[longest]
    return drawn.at[tuple(spot)].set(largest)


def steps_of(stream_key, dims, cuts, low, high):
    factor_of, own = 1.0, jax.random.fold_in(stream_key, 6)
    for axis_at, blocks in cuts:
        draws = jnp.exp(jax.random.uniform(jax.random.fold_in(own, axis_at), (blocks,), jnp.float32, low / len(cuts), high / len(cuts)))
        factor_of = factor_of * jnp.repeat(draws, dims[axis_at] // blocks).reshape([-1 if axis == axis_at else 1 for axis in range(len(dims))])
    return factor_of


def noise(own_key, dims, width, limit, cuts=(), dtype=jnp.bfloat16):
    entries = width * jax.random.normal(own_key, dims, jnp.float32)
    if cuts:
        entries = entries * steps_of(own_key, dims, cuts, -0.22, 0.18)
    return jnp.clip(entries, -limit, limit).astype(dtype)


def setup_inputs(seed: int = 0, part: int = 0) -> dict:
    seeds = jax.random.split(jax.random.key(seed), 9)
    own_keys = jax.random.split(jax.random.fold_in(seeds[8], part), 9)
    video_features = noise(own_keys[0], (T_SIZE, H, W, C), 1.0, 6.0, ((0, 16),))
    cotangent = noise(own_keys[1], (T_SIZE, H, W, C), 1.0, 6.0, ((0, 16),))
    encoder_weight = noise(seeds[2], (27 * C, C), (27 * C) ** -0.5, 0.078125)
    down_weight = noise(seeds[3], (8 * C, C), (8 * C) ** -0.5, 0.125)
    coarse_weight = noise(seeds[4], (3 * C, C), (3 * C) ** -0.5, 0.21875)
    up_weight = noise(seeds[5], (C, 8 * C), C ** -0.5, 0.375)
    decoder_weight = noise(seeds[6], (27 * C, C), (27 * C) ** -0.5, 0.078125)
    levels = place_ends(jax.random.randint(seeds[7], (C,), 3, 9), jax.random.fold_in(seeds[7], 1), 3, 8).astype(jnp.int32)
    return {"video_features": video_features, "cotangent": cotangent, "encoder_weight": encoder_weight, "down_weight": down_weight, "coarse_weight": coarse_weight, "up_weight": up_weight, "decoder_weight": decoder_weight, "levels": levels}


two_pi = 2.0 * math.pi

def tap_rows(padded, frames, tile_rows, tile_cols):
    pieces = [padded[step_t:step_t + frames, step_r:step_r + tile_rows, step_c:step_c + tile_cols] for step_t in range(3) for step_r in range(3) for step_c in range(3)]
    return jnp.concatenate(pieces, axis=-1).reshape(frames * tile_rows * tile_cols, -1)

def flip_taps(weight, count):
    channels = weight.shape[1]
    blocks = weight.reshape(count, channels, channels)[::-1]
    return jnp.transpose(blocks, (0, 2, 1)).reshape(count * channels, channels)

def to_depth(field):
    frames, tile_rows, tile_cols, channels = field.shape
    split = field.reshape(frames // 2, 2, tile_rows // 2, 2, tile_cols // 2, 2, channels)
    return jnp.transpose(split, (0, 2, 4, 1, 3, 5, 6)).reshape(frames // 2, tile_rows // 2, tile_cols // 2, 8 * channels)

def from_depth(field):
    frames, tile_rows, tile_cols, packed = field.shape
    channels = packed // 8
    split = field.reshape(frames, tile_rows, tile_cols, 2, 2, 2, channels)
    return jnp.transpose(split, (0, 3, 1, 4, 2, 5, 6)).reshape(2 * frames, 2 * tile_rows, 2 * tile_cols, channels)

def transposed_product(left, right):
    return lax.dot_general(left, right, (((0,), (0,)), ((), ())), preferred_element_type=jnp.float32)

def product_with_transpose(left, right):
    return lax.dot_general(left, right, (((1,), (1,)), ((), ())), preferred_element_type=jnp.float32)

def time_columns(padded, frames):
    channels = padded.shape[-1]
    pieces = [padded[step_t:step_t + frames] for step_t in range(3)]
    return jnp.concatenate(pieces, axis=-1).reshape(-1, 3 * channels)

def reference(video_features, cotangent, encoder_weight, down_weight, coarse_weight, up_weight, decoder_weight, levels):
    frames, tile_rows, tile_cols, channels = video_features.shape
    fine_shape = video_features.shape
    grad_scale = 1.0 / math.sqrt(frames * tile_rows * tile_cols)
    half_range = (levels.astype(jnp.float32) - 1.0) * 0.5
    spatial = ((1, 1), (1, 1), (0, 0))
    past_pad = ((2, 0),) + spatial
    later_pad = ((0, 2),) + spatial
    enc_patches = tap_rows(jnp.pad(video_features, past_pad), frames, tile_rows, tile_cols)
    pre_enc = jnp.dot(enc_patches, encoder_weight, preferred_element_type=jnp.float32).reshape(fine_shape)
    hidden = (video_features.astype(jnp.float32) + jax.nn.silu(pre_enc)).astype(jnp.bfloat16)
    stacked = to_depth(hidden)
    coarse_shape = stacked.shape[:3] + (channels,)
    packed_shape = stacked.shape
    stacked_rows = stacked.reshape(-1, 8 * channels)
    latent = jnp.dot(stacked_rows, down_weight, preferred_element_type=jnp.float32).astype(jnp.bfloat16).reshape(coarse_shape)
    coarse_frames = coarse_shape[0]
    time_pad = ((2, 0), (0, 0), (0, 0), (0, 0))
    time_later = ((0, 2), (0, 0), (0, 0), (0, 0))
    latent_columns = time_columns(jnp.pad(latent, time_pad), coarse_frames)
    pre_code = jnp.dot(latent_columns, coarse_weight, preferred_element_type=jnp.float32)
    squashed = jnp.tanh(pre_code)
    bounded = half_range * squashed
    latent_codes = ((bounded - jnp.sin(two_pi * bounded) / two_pi) / half_range).astype(jnp.bfloat16)
    later_cot = tap_rows(jnp.pad(cotangent, later_pad), frames, tile_rows, tile_cols)
    back_dec = jnp.dot(later_cot, flip_taps(decoder_weight, 27), preferred_element_type=jnp.float32).reshape(fine_shape)
    decoded_grad = (cotangent.astype(jnp.float32) + back_dec).astype(jnp.bfloat16)
    depth_grad = to_depth(decoded_grad).reshape(-1, 8 * channels)
    code_grad = product_with_transpose(depth_grad, up_weight).astype(jnp.bfloat16)
    pre_grad = (code_grad.astype(jnp.float32) * (1.0 - jnp.cos(two_pi * bounded)) * (1.0 - squashed * squashed)).astype(jnp.bfloat16)
    later_columns = time_columns(jnp.pad(pre_grad.reshape(coarse_shape), time_later), coarse_frames)
    latent_grad = jnp.dot(later_columns, flip_taps(coarse_weight, 3), preferred_element_type=jnp.float32).astype(jnp.bfloat16)
    hidden_grad = from_depth(product_with_transpose(latent_grad, down_weight).reshape(packed_shape))
    sigmoid_pre = jax.nn.sigmoid(pre_enc)
    enc_pre_grad = (hidden_grad * sigmoid_pre * (1.0 + pre_enc * (1.0 - sigmoid_pre))).astype(jnp.bfloat16)
    later_enc = tap_rows(jnp.pad(enc_pre_grad, later_pad), frames, tile_rows, tile_cols)
    back_enc = jnp.dot(later_enc, flip_taps(encoder_weight, 27), preferred_element_type=jnp.float32).reshape(fine_shape)
    video_grad = (hidden_grad + back_enc).astype(jnp.bfloat16)
    down_grad = transposed_product(stacked_rows, latent_grad) * grad_scale
    coarse_grad = transposed_product(latent_columns, pre_grad) * grad_scale
    up_grad = transposed_product(latent_codes, depth_grad) * grad_scale
    return (video_grad, latent_codes.reshape(coarse_shape), down_grad, coarse_grad, up_grad)
```

```python
import math

import jax
import jax.numpy as jnp
from jax import lax
from jax.sharding import PartitionSpec as P

two_pi = 2.0 * math.pi


def from_behind(value, axis, steps):
    count = lax.axis_size(axis)
    leading, last = (max(0, -steps), min(count, count - steps))
    return lax.ppermute(value, axis, [(source, source + steps) for source in range(leading, last)])


def tap_rows(padded, frames, tile_rows, tile_cols):
    pieces = [
        padded[step_t : step_t + frames, step_r : step_r + tile_rows, step_c : step_c + tile_cols]
        for step_t in range(3)
        for step_r in range(3)
        for step_c in range(3)
    ]
    return jnp.concatenate(pieces, axis=-1).reshape(frames * tile_rows * tile_cols, -1)


def flip_taps(weight, count):
    channels = weight.shape[1]
    blocks = weight.reshape(count, channels, channels)[::-1]
    return jnp.transpose(blocks, (0, 2, 1)).reshape(count * channels, channels)


def to_depth(field):
    frames, tile_rows, tile_cols, channels = field.shape
    split = field.reshape(frames // 2, 2, tile_rows // 2, 2, tile_cols // 2, 2, channels)
    return jnp.transpose(split, (0, 2, 4, 1, 3, 5, 6)).reshape(
        frames // 2, tile_rows // 2, tile_cols // 2, 8 * channels
    )


def from_depth(field):
    frames, tile_rows, tile_cols, packed = field.shape
    channels = packed // 8
    split = field.reshape(frames, tile_rows, tile_cols, 2, 2, 2, channels)
    return jnp.transpose(split, (0, 3, 1, 4, 2, 5, 6)).reshape(
        2 * frames, 2 * tile_rows, 2 * tile_cols, channels
    )


def transposed_product(left, right):
    return lax.dot_general(
        left, right, (((0,), (0,)), ((), ())), preferred_element_type=jnp.float32
    )


def product_with_transpose(left, right):
    return lax.dot_general(
        left, right, (((1,), (1,)), ((), ())), preferred_element_type=jnp.float32
    )


def time_columns(padded, frames):
    channels = padded.shape[-1]
    pieces = [padded[step_t : step_t + frames] for step_t in range(3)]
    return jnp.concatenate(pieces, axis=-1).reshape(-1, 3 * channels)


def spatial_pad(field):
    return jnp.pad(field, ((0, 0), (1, 1), (1, 1), (0, 0)))


def fine_patches(field):
    frames, tile_rows, tile_cols, channels = field.shape
    earlier = from_behind(field, "tm", 1)
    joined = jnp.concatenate([earlier, field], axis=0)
    return tap_rows(spatial_pad(joined), frames, tile_rows, tile_cols)


def fine_future(grad_field, weight):
    frames, tile_rows, tile_cols, channels = grad_field.shape
    later_frames = from_behind(grad_field, "tm", -1)
    joined = jnp.concatenate([grad_field, later_frames], axis=0)
    patches = tap_rows(spatial_pad(joined), frames, tile_rows, tile_cols)
    return jnp.dot(patches, flip_taps(weight, 27), preferred_element_type=jnp.float32).reshape(
        grad_field.shape
    )


def quantize(padded, frames, coarse_weight, half_range):
    columns = time_columns(padded, frames)
    pre_code = jnp.dot(columns, coarse_weight, preferred_element_type=jnp.float32)
    squashed = jnp.tanh(pre_code)
    bounded = half_range * squashed
    code_values = ((bounded - jnp.sin(two_pi * bounded) / two_pi) / half_range).astype(jnp.bfloat16)
    return (code_values, (columns, squashed, bounded))


def code_backward(code_grad, state):
    columns, squashed, bounded = state
    factor = (1.0 - jnp.cos(two_pi * bounded)) * (1.0 - squashed * squashed)
    return (code_grad.astype(jnp.float32) * factor).astype(jnp.bfloat16)


def coarse_earlier(latent):
    frames = latent.shape[0]
    shift_count = (frames + 1) // frames
    pieces = [from_behind(latent, "tm", lag_dev) for lag_dev in range(shift_count, 0, -1)]
    joined = jnp.concatenate(pieces + [latent], axis=0)
    return joined


def coarse_later(field):
    frames = field.shape[0]
    shift_count = (frames + 1) // frames
    pieces = [from_behind(field, "tm", -lag_dev) for lag_dev in range(1, shift_count + 1)]
    joined = jnp.concatenate([field] + pieces, axis=0)
    return joined


def spread_forward(latent, coarse_weight, half_range):
    code_values, state = quantize(
        coarse_earlier(latent), latent.shape[0], coarse_weight, half_range
    )
    return (code_values.reshape(latent.shape), state)


def spread_backward(code_field, state, coarse_weight):
    frames = code_field.shape[0]
    channels = code_field.shape[-1]
    pre_grad = code_backward(code_field.reshape(-1, channels), state)
    later_cols = time_columns(coarse_later(pre_grad.reshape(code_field.shape)), frames)
    latent_grad = jnp.dot(
        later_cols, flip_taps(coarse_weight, 3), preferred_element_type=jnp.float32
    ).astype(jnp.bfloat16)
    return (latent_grad.reshape(code_field.shape), pre_grad)


def shards(
    video_features,
    cotangent,
    encoder_weight,
    down_weight,
    coarse_weight,
    up_weight,
    decoder_weight,
    levels,
):
    frames, tile_rows, tile_cols, channels = video_features.shape
    grad_scale = 1.0 / math.sqrt(frames * lax.axis_size("tm") * tile_rows * tile_cols)
    half_range = (levels.astype(jnp.float32) - 1.0) * 0.5
    enc_patches = fine_patches(video_features)
    pre_enc = jnp.dot(enc_patches, encoder_weight, preferred_element_type=jnp.float32).reshape(
        video_features.shape
    )
    hidden = (video_features.astype(jnp.float32) + jax.nn.silu(pre_enc)).astype(jnp.bfloat16)
    stacked = to_depth(hidden)
    packed_shape = stacked.shape
    coarse_shape = packed_shape[:3] + (channels,)
    stacked_rows = stacked.reshape(-1, 8 * channels)
    latent = (
        jnp.dot(stacked_rows, down_weight, preferred_element_type=jnp.float32)
        .astype(jnp.bfloat16)
        .reshape(coarse_shape)
    )
    latent_codes, coarse_state = spread_forward(latent, coarse_weight, half_range)
    code_rows = latent_codes.reshape(-1, channels)
    back_dec = fine_future(cotangent, decoder_weight)
    decoded_grad = (cotangent.astype(jnp.float32) + back_dec).astype(jnp.bfloat16)
    depth_grad = to_depth(decoded_grad).reshape(-1, 8 * channels)
    code_grad = product_with_transpose(depth_grad, up_weight).astype(jnp.bfloat16)
    code_field = code_grad.reshape(coarse_shape)
    latent_grad, pre_grad = spread_backward(code_field, coarse_state, coarse_weight)
    latent_rows = latent_grad.reshape(-1, channels)
    hidden_grad = from_depth(product_with_transpose(latent_rows, down_weight).reshape(packed_shape))
    sigmoid_pre = jax.nn.sigmoid(pre_enc)
    enc_pre_grad = (hidden_grad * sigmoid_pre * (1.0 + pre_enc * (1.0 - sigmoid_pre))).astype(
        jnp.bfloat16
    )
    back_enc = fine_future(enc_pre_grad, encoder_weight)
    video_grad = (hidden_grad + back_enc).astype(jnp.bfloat16)
    count = lax.axis_size("tm")

    def slices(rows):
        return rows.reshape(rows.shape[0], count, -1).transpose(1, 0, 2)

    left = jnp.concatenate(
        [slices(stacked_rows), slices(coarse_state[0]), slices(code_rows)], axis=-1
    )
    left = lax.all_to_all(left, "tm", 0, 0, tiled=True)
    left = left.reshape(-1, left.shape[-1])
    right = lax.all_gather(jnp.concatenate([latent_rows, pre_grad], axis=-1), "tm", tiled=True)
    depth_all = lax.all_gather(depth_grad, "tm", tiled=True)
    down_cols = stacked_rows.shape[1] // count
    coarse_cols = coarse_state[0].shape[1] // count
    down_grad = transposed_product(left[:, :down_cols], right[:, :channels]) * grad_scale
    coarse_grad = (
        transposed_product(left[:, down_cols : down_cols + coarse_cols], right[:, channels:])
        * grad_scale
    )
    up_grad = transposed_product(left[:, down_cols + coarse_cols :], depth_all) * grad_scale
    return (video_grad, latent_codes, down_grad, coarse_grad, up_grad)


def solution(mesh):
    placed = (P("tm", "grp", None, None), P("tm", "grp", None, None), P(), P(), P(), P(), P(), P())
    return jax.shard_map(
        shards,
        mesh=mesh,
        in_specs=placed,
        out_specs=(
            P("tm", "grp", None, None),
            P("tm", "grp", None, None),
            P(("grp", "tm"), None),
            P(("grp", "tm"), None),
            P(("grp", "tm"), None),
        ),
        check_vma=False,
    )
```
